32 devices in a mesh: grp: 2 (over y), row: 4 (over z), col: 4 (over x, core).
Axes of the slice: x: 2, y: 2, z: 4, core: 2. Of those that a mesh axis runs over, the one named last changes fastest.
Arguments:
- hessian_old: float32 [18432, 9216], P(('grp', 'row'), 'col'), parts along dimension 0, may hold values from -8 to 48, as said below
- tokens: bfloat16 [128, 9216], P(('grp', 'row'), 'col'), parts along dimension 0, may hold values from -6 to 6
- weight: float32 [128, 9216], P(('grp', 'row'), 'col'), parts along dimension 0, may hold values from -6 to 6
- dense_weight: float32 [128, 9216], P(('grp', 'row'), 'col'), parts along dimension 0, may hold values from -6 to 6
- block_mask: int32 [128, 72], P(('grp', 'row'), 'col'), parts along dimension 0, may hold values 0 or 1
Outputs:
- hessian: float32 [18432, 9216], P(('grp', 'row'), 'col'), parts along dimension 0
- new_weight: float32 [128, 9216], P(('grp', 'row'), 'col'), parts along dimension 0
The draws below stay inside these ranges and needn't reach their ends.
There are 2 independent parts, one for each index of `grp`. The reference program is written for one: setup_inputs(seed, part) draws one part's arguments, and reference() takes and returns one part's arrays. A program takes and returns all parts, laid end to end along the dimension named above; each array names one. Nothing has to cross between parts.
Inputs may be any that keep to these rules, and one draw needn't show every extreme that they name: hessian_old is symmetric and has a positive diagonal.
All inputs are finite; a program needn't handle non-finite values. No bound on the sum of `block_mask` on one device may be relied on, other than what follows from the above.
Results may differ from the reference program's by a relative error of at most 0.0035.
Values may be sent and summed in bfloat16 or wider, within the bound.
A program may use at most 128 MiB of HBM per device.

```python
import jax
import jax.numpy as jnp

W = 9216
BLOCK = 128
TOKENS = 64
R = 64
BLOCKS = 72


def draw_hessian_old(key, part):
    key_off = jax.random.fold_in(key, 11)
    key_diag = jax.random.fold_in(key, 12)
    loose = jax.random.normal(key_off, (W, W), jnp.float32) * 0.05
    symmetric = loose + loose.T
    diagonal_values = 0.5 * jnp.exp(jax.random.uniform(key_diag, (W,), jnp.float32, 0.0, jnp.log(8.0)))
    positions = jnp.arange(W)
    symmetric = symmetric.at[positions, positions].set(diagonal_values)
    return symmetric.astype(jnp.float32)


def plant(array, key, least, largest):
    longest = array.shape.index(max(array.shape))
    spots = []
    for shift in (0, 1):
        where = [jax.random.randint(jax.random.fold_in(key, axis), (), 0, length) for axis, length in enumerate(array.shape)]
        where[longest] = (where[longest] + shift) % array.shape[longest]
        spots.append(tuple(where))
    return array.at[spots[0]].set(least).at[spots[1]].set(largest)


def steps_of(stream_key, dims, cuts, least, high):
    def one(position, blocks):
        heights = jax.random.uniform(jax.random.fold_in(jax.random.fold_in(stream_key, 6), position), (blocks,), jnp.float32, least / len(cuts), high / len(cuts))
        return jnp.repeat(jnp.exp(heights), dims[position] // blocks).reshape((-1,) + (1,) * (len(dims) - position - 1))

    level = one(*cuts[0])
    for cut in cuts[1:]:
        level = level * one(*cut)
    return level


def scatter_about(own_key, dims, scale, bound, cuts=(), held_as=jnp.bfloat16):
    level = steps_of(own_key, dims, cuts, -0.22, 0.18) if cuts else 1.0
    entries = jax.random.normal(own_key, dims, jnp.float32) * scale * level
    return jnp.minimum(jnp.maximum(entries, -bound), bound).astype(held_as)


def setup_inputs(seed: int = 0, part: int = 0) -> dict:
    seeds = jax.random.split(jax.random.key(seed), 6)
    part_keys = jax.random.split(jax.random.fold_in(seeds[5], part), 6)
    hessian_old = draw_hessian_old(jax.random.fold_in(jax.random.fold_in(seeds[5], part), 71), part)
    tokens = scatter_about(part_keys[1], (TOKENS, W), 1.0, 6.0, ((0, 4), (1, 4)))
    weight = scatter_about(part_keys[2], (R, W), 1.0, 6.0, ((0, 4), (1, 4)), jnp.float32)
    dense_weight = scatter_about(part_keys[3], (R, W), 1.0, 6.0, ((0, 4), (1, 4)), jnp.float32)
    block_mask = plant((jax.random.randint(part_keys[4], (R, BLOCKS), 0, 2) < 1).astype(jnp.int32), jax.random.fold_in(part_keys[4], 1), 0, 1)
    return {"hessian_old": hessian_old, "tokens": tokens, "weight": weight, "dense_weight": dense_weight, "block_mask": block_mask}


def reference(hessian_old, tokens, weight, dense_weight, block_mask):
    gram_tile = jnp.dot(tokens.T, tokens, preferred_element_type=jnp.float32)
    hessian = hessian_old + gram_tile / TOKENS
    kept_mask = jnp.repeat(block_mask.astype(jnp.float32), BLOCK, axis=1)
    difference = (kept_mask * weight - dense_weight).astype(jnp.bfloat16)
    hess_low = hessian.astype(jnp.bfloat16)
    gradient = jnp.dot(difference, hess_low, preferred_element_type=jnp.float32)
    diag_sum = jnp.trace(hessian)
    step_size = 0.25 * W / diag_sum
    new_weight = kept_mask * (weight - step_size * gradient)
    return hessian, new_weight
```

```python
import functools

import jax
import jax.numpy as jnp
from jax import lax
from jax.experimental import pallas as pl
from jax.experimental.pallas import tpu as pltpu
from jax.sharding import PartitionSpec as P

MESH = pl.DeviceIdType.MESH


def general(hessian_old, tokens, weight, dense_weight, block_mask):
    row_tile = hessian_old.shape[0]
    col_tile = hessian_old.shape[1]
    row_idx = lax.axis_index("row")
    col_idx = lax.axis_index("col")
    col_panel = lax.all_gather(tokens, "row", axis=0, tiled=True)
    features = lax.all_gather(tokens, "col", axis=1, tiled=True)
    row_panel = lax.all_to_all(features, "row", split_axis=1, concat_axis=0, tiled=True)
    gram_tile = lax.dot_general(
        row_panel, col_panel, (((0,), (0,)), ((), ())), preferred_element_type=jnp.float32
    )
    token_count = tokens.shape[0] * lax.axis_size("row")
    hessian = hessian_old + gram_tile / token_count
    row_ids = lax.broadcasted_iota(jnp.int32, (row_tile, col_tile), 0) + row_idx * row_tile
    col_ids = lax.broadcasted_iota(jnp.int32, (row_tile, col_tile), 1) + col_idx * col_tile
    local_trace = jnp.sum(jnp.where(row_ids == col_ids, hessian, jnp.float32(0.0)))
    diag_sum = lax.psum(local_trace, ("row", "col"))
    weight_rows = weight.shape[0]
    block_count = block_mask.shape[1]
    block_width = col_tile // block_count
    kept_mask = (
        block_mask.astype(jnp.float32)[:, :, None] * jnp.ones((1, 1, block_width), jnp.float32)
    ).reshape(weight_rows, col_tile)
    difference = (kept_mask * weight - dense_weight).astype(jnp.bfloat16)
    hess_low = hessian.astype(jnp.bfloat16)
    partial_grad = lax.dot_general(
        lax.all_gather(difference, "row", axis=0, tiled=True),
        hess_low,
        (((1,), (1,)), ((), ())),
        preferred_element_type=jnp.float32,
    )
    spread = lax.all_to_all(partial_grad, "row", split_axis=0, concat_axis=1, tiled=True)
    gradient = lax.psum_scatter(spread, "col", scatter_dimension=1, tiled=True)
    step_size = 0.25 * (row_tile * lax.axis_size("row")) / diag_sum
    new_weight = kept_mask * (weight - step_size * gradient)
    return (hessian, new_weight)


def hail(devices):
    barrier = pltpu.get_barrier_semaphore()
    for device in devices:
        pl.semaphore_signal(barrier, inc=1, device_id=device, device_id_type=MESH)


def meet(count):
    pl.semaphore_wait(pltpu.get_barrier_semaphore(), count)


def remote(src, dst, send_sem, recv_sem, device):
    return pltpu.make_async_remote_copy(
        src_ref=src, dst_ref=dst, send_sem=send_sem, recv_sem=recv_sem,
        device_id=device, device_id_type=MESH,
    )


def scaled(value, count):
    exact = count & (count - 1) == 0
    return value * (1.0 / count) if exact else value / count


def exchange_kernel(
    n, parts, old_hbm, tok_hbm, w_hbm, d_hbm, m_hbm,
    old, colp, rowt, gsum, mgot, tgot,
    tok_ref, w_ref, d_ref, m_ref, diff, cold, part, pout, pgot, gred, mine, trow, tsum,
    in_sem, old_sem, send_l, recv_l, relay_l, send_x, recv_x, send_p, recv_p, send_f, recv_f,
    send_m, recv_m, send_t, recv_t, send_u, recv_u,
):
    g, r, c = lax.axis_index("grp"), lax.axis_index("row"), lax.axis_index("col")
    tile = old.shape[0]
    depth = diff.shape[0]
    held = tok_ref.shape[0]
    span = tile // parts
    loads = [
        pltpu.make_async_copy(src, dst, in_sem.at[i])
        for i, (src, dst) in enumerate([(w_hbm, w_ref), (d_hbm, d_ref), (m_hbm, m_ref), (tok_hbm, tok_ref)])
    ]
    for load in loads:
        load.start()
    stripes = [slice(p * span, (p + 1) * span) for p in range(parts)]
    olds = [
        pltpu.make_async_copy(old_hbm.at[at, :], old.at[at, :], old_sem.at[p])
        for p, at in enumerate(stripes)
    ]
    for load in olds:
        load.start()
    others = [lax.rem(r + j, n) for j in range(1, n)]
    beside = [lax.rem(c + j, n) for j in range(1, n)]
    hail([(g, rr, c) for rr in others] + [(g, r, cc) for cc in beside])
    for load in loads[:3]:
        load.wait()
    blocks = m_ref.shape[1]
    width = tile // blocks
    for b in range(blocks):
        at = slice(b * width, (b + 1) * width)
        kept = m_ref[:, b : b + 1].astype(jnp.float32)
        diff[:, at] = (kept * w_ref[:, at] - d_ref[:, at]).astype(jnp.bfloat16)
    meet(len(others) + len(beside))

    root = r == c
    partner = c + 1 - 2 * lax.rem(c, 2)
    twins = [lax.rem(c + 2 * j, n) for j in range(1, n // 2)]
    even = lax.rem(r, 2) == lax.rem(c, 2)
    hops = [(k, sign) for k in range(max(n - 2, 1), 0, -1) for sign in (1, -1)]
    any_dev = (g, r, partner)

    def line(kind, src, panel, act):
        for i, (k, sign) in enumerate(hops):
            dest = r + sign * k
            copy = remote(src, panel.at[r], send_l.at[kind, i], recv_l.at[kind, r], (g, dest, c))

            @pl.when(jnp.logical_and(dest >= 0, dest < n))
            def _():
                act(copy)

    def got_line(kind, panel, s):
        remote(panel.at[s], panel.at[s], send_l.at[kind, 0], recv_l.at[kind, s], any_dev).wait_recv()

    def relay(kind, panel, act):
        if n == 2:
            return
        for at, s, dest in ((1, n - 1, 0), (n - 2, 0, n - 1)):
            copy = remote(panel.at[s], panel.at[s], relay_l.at[kind], recv_l.at[kind, s], (g, dest, c))

            @pl.when(r == at)
            def _():
                act(copy, s)

    def pass_on(kind, panel):
        def act(copy, s):
            got_line(kind, panel, s)
            copy.start()

        relay(kind, panel, act)

    def across(s, src, act):
        for i, cc in enumerate(twins + [partner]):
            act(remote(src, rowt.at[s], send_x.at[i, s], recv_x.at[s], (g, r, cc)))

    def down(s, act):
        act(remote(rowt.at[s], rowt.at[s], send_x.at[0, s], recv_x.at[s], any_dev))

    def got_x(s):
        down(s, lambda copy: copy.wait_recv())

    start = lambda copy: copy.start()
    sent = lambda copy: copy.wait_send()
    line(0, diff, cold, start)
    loads[3].wait()
    line(1, tok_ref, colp, start)

    @pl.when(root)
    def _():
        across(r, tok_ref, start)

    cold[r] = diff[...]
    colp[r] = tok_ref[...]
    total = jnp.zeros((held, width), jnp.float32)
    for b in range(blocks):
        value = tok_ref[:, b * width : (b + 1) * width].astype(jnp.float32)
        total = total + value * value
    total = jnp.sum(total.reshape(held // 8, 8, width), axis=0)
    tsum[...] = scaled(total, n * held)

    pass_on(0, cold)

    def near(s):
        if n == 2:
            return True
        far = jnp.logical_or(jnp.logical_and(r == 1, s == n - 1), jnp.logical_and(r == n - 2, s == 0))
        return jnp.logical_not(far)

    def got_panel(kind, panel, s):
        @pl.when(near(s))
        def _():
            got_line(kind, panel, s)

    for s in others:
        got_panel(0, cold, s)

    same = lax.broadcasted_iota(jnp.int32, (width, width), 0) == lax.broadcasted_iota(
        jnp.int32, (width, width), 1
    )

    def piece(p, cc, act):
        at = stripes[p]
        i = lax.rem(cc - c + n, n) - 1
        act(remote(
            pout.at[cc, :, at], pgot.at[c, :, at], send_p.at[p, i], recv_p.at[p, c], (g, r, cc)
        ))

    def multiply(p):
        at = stripes[p]
        olds[p].wait()
        value = lax.dot_general(
            old[at, :].astype(jnp.bfloat16), cold[...].reshape(n * depth, tile), (((1,), (1,)), ((), ())),
            preferred_element_type=jnp.float32,
        ).T.reshape(n, depth, span)
        part[:, :, at] = value
        pout[:, :, at] = value.astype(jnp.bfloat16)
        for cc in beside:
            piece(p, cc, start)

        @pl.when(root)
        def _():
            for b in range(p * span // width, (p + 1) * span // width):
                at = slice(b * width, (b + 1) * width)
                diag = jnp.where(same, old[at, at], 0.0)
                tsum[...] += jnp.sum(diag.reshape(width // 8, 8, width), axis=0)

    def owner(p):
        at = stripes[p]
        return remote(gred.at[:, at], gsum.at[:, at], send_f.at[p], recv_f.at[p], (g, c, r))

    def reduce(p):
        at = stripes[p]
        for cc in beside:
            remote(pout.at[cc, :, at], pgot.at[cc, :, at], send_p.at[p, 0], recv_p.at[p, cc], any_dev).wait_recv()
        value = part[c, :, at]
        for cc in beside:
            value = value + pgot[cc, :, at].astype(jnp.float32)
        gred[:, at] = value.astype(jnp.bfloat16)

        @pl.when(root)
        def _():
            gsum[:, at] = value.astype(jnp.bfloat16)

        @pl.when(jnp.logical_not(root))
        def _():
            owner(p).start()

    def spread_root(order):
        @pl.when(root)
        def _():
            for s in order:
                got_panel(1, colp, s)
                across(s, colp.at[s], start)

    def spread_twin(order):
        @pl.when(jnp.logical_and(even, jnp.logical_not(root)))
        def _():
            for s in order:
                got_x(s)
                down(s, start)

    multiply(0)
    pass_on(1, colp)
    for p in range(1, parts):
        multiply(p)
    spread_root(others)
    spread_twin([r] + others)
    trace_row = [remote(tsum, trow.at[c], send_t.at[i], recv_t.at[c], (g, r, cc)) for i, cc in enumerate(beside)]
    for copy in trace_row:
        copy.start()
    trow[c] = tsum[...]
    for p in range(parts - 1):
        reduce(p)

    @pl.when(jnp.logical_not(root))
    def _():
        for s in others:
            got_panel(1, colp, s)

    mine[...] = jnp.zeros_like(mine)
    mine[:, : n * held] = lax.dot_general(
        diff[...], colp[...].reshape(n * held, tile), (((1,), (1,)), ((), ())),
        preferred_element_type=jnp.float32,
    )
    cross = [remote(mine, mgot.at[c], send_m.at[i], recv_m.at[c], (g, r, cc)) for i, cc in enumerate(beside)]
    for copy in cross:
        copy.start()
    mgot[c] = mine[...]
    for cc in beside:
        remote(tsum, trow.at[cc], send_t.at[0], recv_t.at[cc], any_dev).wait_recv()
    total = jnp.zeros(tsum.shape, jnp.float32)
    for cc in range(n):
        total = total + trow[cc]
    tgot[r] = total
    trace_col = [remote(tgot.at[r], tgot.at[r], send_u.at[i], recv_u.at[r], (g, rr, c)) for i, rr in enumerate(others)]
    for copy in trace_col:
        copy.start()
    reduce(parts - 1)

    @pl.when(root)
    def _():
        for s in range(n):
            rowt[s] = colp[s]

    @pl.when(jnp.logical_not(jnp.logical_or(root, even)))
    def _():
        for s in range(n):
            got_x(s)

    for cc in beside:
        remote(mine, mgot.at[cc], send_m.at[0], recv_m.at[cc], any_dev).wait_recv()
    for rr in others:
        remote(tsum, tgot.at[rr], send_u.at[0], recv_u.at[rr], any_dev).wait_recv()

    @pl.when(jnp.logical_not(root))
    def _():
        for p in range(parts):
            owner(p).wait_recv()

    for kind, src, panel in ((0, diff, cold), (1, tok_ref, colp)):
        line(kind, src, panel, sent)
        relay(kind, panel, lambda copy, s: copy.wait_send())

    @pl.when(root)
    def _():
        across(r, tok_ref, sent)
        for s in others:
            across(s, colp.at[s], sent)

    @pl.when(jnp.logical_and(even, jnp.logical_not(root)))
    def _():
        for s in range(n):
            down(s, sent)

    for p in range(parts):
        for cc in beside:
            piece(p, cc, sent)

    @pl.when(jnp.logical_not(root))
    def _():
        for p in range(parts):
            owner(p).wait_send()

    for copy in trace_row + cross + trace_col:
        copy.wait_send()


def main_kernel(
    n, rows, old_ref, rt_ref, cp_ref, g_ref, mix_ref, trace_ref, w_ref, m_ref, out_hbm, new_hbm,
    out, new, out_sem, new_sem,
):
    tile = old_ref.shape[0]
    tokens = rt_ref.shape[0]
    steps = tile // rows
    slots = out.shape[0]

    def store(i):
        return pltpu.make_async_copy(
            out.at[lax.rem(i, slots)],
            out_hbm.at[pl.ds(pl.multiple_of(i * rows, rows), rows), :],
            out_sem.at[lax.rem(i, slots)],
        )

    @pl.loop(0, steps)
    def _(i):
        slot = lax.rem(i, slots)

        @pl.when(i >= slots)
        def _():
            store(i - slots).wait()

        here = pl.ds(pl.multiple_of(i * rows, rows), rows)
        gram = lax.dot_general(
            rt_ref[:, here], cp_ref[...], (((0,), (0,)), ((), ())), preferred_element_type=jnp.float32
        )
        out[slot] = old_ref[here, :] + scaled(gram, tokens)
        store(i).start()

    total = jnp.zeros(trace_ref.shape[1:], jnp.float32)
    for s in range(n):
        total = total + trace_ref[s]
    step = 0.25 * (tile * n) / jnp.sum(total, axis=(0, 1), keepdims=True)
    mix = jnp.zeros(mix_ref.shape[1:], jnp.float32)
    for s in range(n):
        mix = mix + mix_ref[s]
    mix = mix[:, :tokens]
    high = mix.astype(jnp.bfloat16)
    low = (mix - high.astype(jnp.float32)).astype(jnp.bfloat16)
    both = jnp.concatenate([high, low], axis=0)
    depth = high.shape[0]
    blocks = m_ref.shape[1]
    width = tile // blocks
    for b in range(blocks):
        at = slice(b * width, (b + 1) * width)
        extra = jnp.dot(both, cp_ref[:, at], preferred_element_type=jnp.float32)
        extra = scaled(extra[:depth] + extra[depth:], tokens)
        grad = g_ref[:, at].astype(jnp.float32) + extra
        kept = m_ref[:, b : b + 1].astype(jnp.float32)
        new[:, at] = kept * (w_ref[:, at] - step * grad)
    last = pltpu.make_async_copy(new, new_hbm, new_sem)
    last.start()
    for k in range(min(slots, steps)):
        store(jnp.int32(steps - 1 - k)).wait()
    last.wait()


def fused(n, hessian_old, tokens, weight, dense_weight, block_mask):
    tile = hessian_old.shape[0]
    held = tokens.shape[0]
    depth = weight.shape[0]
    vmem = pl.BlockSpec(memory_space=pltpu.VMEM)
    dma = pltpu.SemaphoreType.DMA
    hbm = pl.BlockSpec(memory_space=pltpu.HBM)
    parts = 3 if tile % 384 == 0 else 1
    wide = -(-n * held // 128) * 128
    old, colp, rowt, gsum, mix, trace = pl.pallas_call(
        functools.partial(exchange_kernel, n, parts),
        out_shape=(
            jax.ShapeDtypeStruct((tile, tile), jnp.float32),
            jax.ShapeDtypeStruct((n, held, tile), jnp.bfloat16),
            jax.ShapeDtypeStruct((n, held, tile), jnp.bfloat16),
            jax.ShapeDtypeStruct((depth, tile), jnp.bfloat16),
            jax.ShapeDtypeStruct((n, depth, wide), jnp.float32),
            jax.ShapeDtypeStruct((n, 8, 128), jnp.float32),
        ),
        in_specs=[hbm] * 5,
        out_specs=(vmem,) * 6,
        scratch_shapes=[
            pltpu.VMEM((held, tile), jnp.bfloat16),
            pltpu.VMEM((depth, tile), jnp.float32),
            pltpu.VMEM((depth, tile), jnp.float32),
            pltpu.VMEM(block_mask.shape, jnp.int32),
            pltpu.VMEM((depth, tile), jnp.bfloat16),
            pltpu.VMEM((n, depth, tile), jnp.bfloat16),
            pltpu.VMEM((n, depth, tile), jnp.float32),
            pltpu.VMEM((n, depth, tile), jnp.bfloat16),
            pltpu.VMEM((n, depth, tile), jnp.bfloat16),
            pltpu.VMEM((depth, tile), jnp.bfloat16),
            pltpu.VMEM((depth, wide), jnp.float32),
            pltpu.VMEM((n, 8, 128), jnp.float32),
            pltpu.VMEM((8, 128), jnp.float32),
            dma((4,)),
            dma((parts,)),
            dma((2, 2 * n)),
            dma((2, n)),
            dma((2,)),
            dma((n // 2, n)),
            dma((n,)),
            dma((parts, n)),
            dma((parts, n)),
            dma((parts,)),
            dma((parts,)),
            dma((n - 1,)),
            dma((n,)),
            dma((n - 1,)),
            dma((n,)),
            dma((n - 1,)),
            dma((n,)),
        ],
        compiler_params=pltpu.CompilerParams(
            collective_id=0, has_side_effects=True, vmem_limit_bytes=16 << 20
        ),
    )(*[pltpu.with_memory_space_constraint(x, pltpu.HBM) for x in (hessian_old, tokens, weight, dense_weight, block_mask)])
    colp = colp.reshape(n * held, tile)
    rowt = rowt.reshape(n * held, tile)
    rows = 256 if tile % 256 == 0 else 128
    hessian, new_weight = pl.pallas_call(
        functools.partial(main_kernel, n, rows),
        out_shape=(
            jax.ShapeDtypeStruct((tile, tile), jnp.float32),
            jax.ShapeDtypeStruct((depth, tile), jnp.float32),
        ),
        in_specs=[vmem] * 8,
        out_specs=(hbm, hbm),
        scratch_shapes=[
            pltpu.VMEM((3, rows, tile), jnp.float32),
            pltpu.VMEM((depth, tile), jnp.float32),
            dma((3,)),
            dma,
        ],
        compiler_params=pltpu.CompilerParams(vmem_limit_bytes=16 << 20),
    )(old, rowt, colp, gsum, mix, trace, weight, block_mask)
    return hessian, new_weight


def solution(mesh):
    n = mesh.shape["row"]

    def on_device(hessian_old, tokens, weight, dense_weight, block_mask):
        tile = hessian_old.shape[0]
        fits = (
            n == mesh.shape["col"]
            and n > 1
            and n % 2 == 0
            and tile == hessian_old.shape[1]
            and tile % 128 == 0
            and tile == block_mask.shape[1] * 128
            and tokens.shape[0] % 16 == 0
            and weight.shape[0] % 16 == 0
        )
        args = (hessian_old, tokens, weight, dense_weight, block_mask)
        return fused(n, *args) if fits else general(*args)

    spec = P(("grp", "row"), "col")
    return jax.shard_map(
        on_device, mesh=mesh, in_specs=(spec,) * 5, out_specs=(spec, spec), check_vma=False
    )
```

```python
import functools

import jax
import jax.numpy as jnp
from jax import lax
from jax.experimental import pallas as pl
from jax.experimental.pallas import tpu as pltpu
from jax.sharding import PartitionSpec as P

MESH = pl.DeviceIdType.MESH


def general(hessian_old, tokens, weight, dense_weight, block_mask):
    row_tile = hessian_old.shape[0]
    col_tile = hessian_old.shape[1]
    row_idx = lax.axis_index("row")
    col_idx = lax.axis_index("col")
    col_panel = lax.all_gather(tokens, "row", axis=0, tiled=True)
    features = lax.all_gather(tokens, "col", axis=1, tiled=True)
    row_panel = lax.all_to_all(features, "row", split_axis=1, concat_axis=0, tiled=True)
    gram_tile = lax.dot_general(
        row_panel, col_panel, (((0,), (0,)), ((), ())), preferred_element_type=jnp.float32
    )
    token_count = tokens.shape[0] * lax.axis_size("row")
    hessian = hessian_old + gram_tile / token_count
    row_ids = lax.broadcasted_iota(jnp.int32, (row_tile, col_tile), 0) + row_idx * row_tile
    col_ids = lax.broadcasted_iota(jnp.int32, (row_tile, col_tile), 1) + col_idx * col_tile
    local_trace = jnp.sum(jnp.where(row_ids == col_ids, hessian, jnp.float32(0.0)))
    diag_sum = lax.psum(local_trace, ("row", "col"))
    weight_rows = weight.shape[0]
    block_count = block_mask.shape[1]
    block_width = col_tile // block_count
    kept_mask = (
        block_mask.astype(jnp.float32)[:, :, None] * jnp.ones((1, 1, block_width), jnp.float32)
    ).reshape(weight_rows, col_tile)
    difference = (kept_mask * weight - dense_weight).astype(jnp.bfloat16)
    hess_low = hessian.astype(jnp.bfloat16)
    partial_grad = lax.dot_general(
        lax.all_gather(difference, "row", axis=0, tiled=True),
        hess_low,
        (((1,), (1,)), ((), ())),
        preferred_element_type=jnp.float32,
    )
    spread = lax.all_to_all(partial_grad, "row", split_axis=0, concat_axis=1, tiled=True)
    gradient = lax.psum_scatter(spread, "col", scatter_dimension=1, tiled=True)
    step_size = 0.25 * (row_tile * lax.axis_size("row")) / diag_sum
    new_weight = kept_mask * (weight - step_size * gradient)
    return (hessian, new_weight)


def hail(devices):
    barrier = pltpu.get_barrier_semaphore()
    for device in devices:
        pl.semaphore_signal(barrier, inc=1, device_id=device, device_id_type=MESH)


def meet(count):
    pl.semaphore_wait(pltpu.get_barrier_semaphore(), count)


def remote(src, dst, send_sem, recv_sem, device):
    return pltpu.make_async_remote_copy(
        src_ref=src, dst_ref=dst, send_sem=send_sem, recv_sem=recv_sem,
        device_id=device, device_id_type=MESH,
    )


def scaled(value, count):
    exact = count & (count - 1) == 0
    return value * (1.0 / count) if exact else value / count


def split(value):
    high = value.astype(jnp.bfloat16)
    return high, value - high.astype(jnp.float32)


def gather_kernel(
    n, parts, old_hbm, tok_hbm, w_hbm, d_hbm, m_hbm, old, colp, rowt, *refs
):
    outs, refs = refs[:n], refs[n:]
    (
        tok_ref, w_ref, d_ref, m_ref, diff, rowd, dsum, pack,
        in_sem, old_sem, send_a, recv_a, send_r, send_d, recv_d, send_x, recv_x, send_s, recv_s,
    ) = refs
    g, r, c = lax.axis_index("grp"), lax.axis_index("row"), lax.axis_index("col")
    tile = old.shape[0]
    held = tok_ref.shape[0]
    depth = diff.shape[0]
    loads = [
        pltpu.make_async_copy(src, dst, in_sem.at[i])
        for i, (src, dst) in enumerate([(w_hbm, w_ref), (d_hbm, d_ref), (m_hbm, m_ref), (tok_hbm, tok_ref)])
    ]
    for load in loads:
        load.start()
    others = [lax.rem(r + j, n) for j in range(1, n)]
    beside = [lax.rem(c + j, n) for j in range(1, n)]
    hail([(g, rr, c) for rr in others] + [(g, r, cc) for cc in beside])
    for load in loads:
        load.wait()
    whole = pltpu.make_async_copy(old_hbm, old, old_sem)
    whole.start()
    blocks = m_ref.shape[1]
    width = tile // blocks
    for b in range(blocks):
        at = slice(b * width, (b + 1) * width)
        kept = m_ref[:, b : b + 1].astype(jnp.float32)
        diff[:, at] = (kept * w_ref[:, at] - d_ref[:, at]).astype(jnp.bfloat16)
    meet(len(others) + len(beside))

    root = r == c
    partner = c + 1 - 2 * lax.rem(c, 2)
    partner_dev = (g, r, partner)
    twins = [lax.rem(c + 2 * j, n) for j in range(1, n // 2)]
    even = lax.rem(r, 2) == lax.rem(c, 2)
    twin = jnp.logical_and(even, jnp.logical_not(root))
    mate = partner
    crosses = r // 2 != c // 2
    panels = (rowd, rowt)
    sources = (diff, tok_ref)
    start = lambda copy: copy.start()
    sent = lambda copy: copy.wait_send()

    def direct(rr):
        return jnp.logical_and(rr != r, jnp.logical_not(jnp.logical_and(crosses, rr == mate)))

    def relay(s, act):
        copy = remote(colp.at[s], colp.at[s], send_r.at[s], recv_a.at[s], (g, mate, c))

        @pl.when(s // 2 != r // 2)
        def _():
            act(copy)

    def token_copy(k):
        rr = lax.rem(c + k, n)
        return rr, remote(tok_ref, colp.at[r], send_a.at[k], recv_a.at[r], (g, rr, c))

    diff_copy = remote(diff, rowd.at[r], send_d, recv_d.at[r], (g, c, c))

    def spread(kind, s, src, act):
        for i, cc in enumerate(twins + [partner]):
            act(remote(src, panels[kind].at[s], send_x.at[i, kind, s], recv_x.at[kind, s], (g, r, cc)))

    def spread_on(kind, s, act):
        at = panels[kind].at[s]
        act(remote(at, at, send_x.at[0, kind, s], recv_x.at[kind, s], partner_dev))

    def got_a(s):
        remote(tok_ref, colp.at[s], send_a.at[0], recv_a.at[s], partner_dev).wait_recv()

    def got_x(kind, s):
        spread_on(kind, s, lambda copy: copy.wait_recv())

    def got_diff(s):
        remote(diff, rowd.at[s], send_d, recv_d.at[s], partner_dev).wait_recv()

    @pl.when(jnp.logical_not(root))
    def _():
        diff_copy.start()
        token_copy(0)[1].start()

    @pl.when(root)
    def _():
        spread(0, r, diff, start)
        spread(1, r, tok_ref, start)

    for k in range(1, n):
        rr, copy = token_copy(k)

        @pl.when(direct(rr))
        def _():
            copy.start()

    colp[r] = tok_ref[...]

    @pl.when(root)
    def _():
        rowd[r] = diff[...]
        for s in others:
            got_diff(s)
            spread(0, s, rowd.at[s], start)

    @pl.when(twin)
    def _():
        for s in [r] + others:
            got_x(0, s)
            spread_on(0, s, start)

    @pl.when(jnp.logical_not(even))
    def _():
        for s in range(n):
            got_x(0, s)

    same = lax.broadcasted_iota(jnp.int32, (width, width), 0) == lax.broadcasted_iota(
        jnp.int32, (width, width), 1
    )

    def diag_to(i, cc):
        return remote(dsum.at[0], dsum.at[1], send_s.at[i], recv_s, (g, r, cc))

    def tokens_step(i):
        s = others[i]

        @pl.when(root)
        def _():
            got_a(s)
            spread(1, s, colp.at[s], start)
            relay(s, start)

        @pl.when(twin)
        def _():
            q = ([r] + others)[i]
            got_x(1, q)
            spread_on(1, q, start)

    whole.wait()
    span = tile // parts
    for p in range(parts):
        at = slice(p * span, (p + 1) * span)
        value = jnp.dot(
            rowd[...].reshape(n * depth, tile), old[:, at].astype(jnp.bfloat16), preferred_element_type=jnp.float32
        )
        pack[:, :, at] = value.astype(jnp.bfloat16).reshape(n, depth, span)
        if p < n - 1:
            tokens_step(p)
    for i in range(parts, n - 1):
        tokens_step(i)

    @pl.when(twin)
    def _():
        got_x(1, others[-1])
        spread_on(1, others[-1], start)

    @pl.when(root)
    def _():
        total = jnp.zeros((8, width), jnp.float32)
        for b in range(blocks):
            at = slice(b * width, (b + 1) * width)
            diag = jnp.where(same, old[at, at], 0.0)
            total = total + jnp.sum(diag.reshape(width // 8, 8, width), axis=0)
        dsum[0] = total
        dsum[1] = total
        for i, cc in enumerate(beside):
            diag_to(i, cc).start()
        for s in range(n):
            rowt[s] = colp[s]

    @pl.when(jnp.logical_not(even))
    def _():
        for s in range(n):
            got_x(1, s)

    mix = lax.dot_general(
        rowd[...].reshape(n * depth, tile), rowt[...].reshape(n * held, tile), (((1,), (1,)), ((), ())),
        preferred_element_type=jnp.float32,
    )
    high, low = split(mix)
    pack[:, :, tile : tile + 2 * n * held] = jnp.concatenate(
        [high.astype(jnp.float32), low], axis=1
    ).astype(jnp.bfloat16).reshape(n, depth, 2 * n * held)
    total = jnp.zeros((n * held, width), jnp.float32)
    for b in range(blocks):
        value = rowt[:, :, b * width : (b + 1) * width].reshape(n * held, width).astype(jnp.float32)
        total = total + value * value
    total = scaled(jnp.sum(total.reshape(n * held // 8, 8, width), axis=0), n * held)

    @pl.when(jnp.logical_not(root))
    def _():
        diag_to(0, partner).wait_recv()

    high, low = split(total + dsum[1])
    both = jnp.concatenate([high.astype(jnp.float32), low], axis=0).astype(jnp.bfloat16)
    for s in range(n):
        pack[s, :, tile + 2 * n * held :] = both
    for k in range(n):
        outs[k][...] = pack[lax.rem(r + k, n)]

    @pl.when(jnp.logical_not(root))
    def _():
        for s in others:
            got_a(s)
        diff_copy.wait_send()
        token_copy(0)[1].wait_send()

    @pl.when(root)
    def _():
        spread(0, r, diff, sent)
        spread(1, r, tok_ref, sent)
        for s in others:
            spread(0, s, rowd.at[s], sent)
            spread(1, s, colp.at[s], sent)
            relay(s, sent)
        for i, cc in enumerate(beside):
            diag_to(i, cc).wait_send()

    @pl.when(twin)
    def _():
        for kind in (0, 1):
            for s in range(n):
                spread_on(kind, s, sent)

    for k in range(1, n):
        rr, copy = token_copy(k)

        @pl.when(direct(rr))
        def _():
            copy.wait_send()


def main_kernel(rows, old_ref, rt_ref, cp_ref, out_hbm, out, out_sem):
    tile = old_ref.shape[0]
    tokens = rt_ref.shape[0]
    steps = tile // rows
    slots = out.shape[0]

    def store(i):
        return pltpu.make_async_copy(
            out.at[lax.rem(i, slots)],
            out_hbm.at[pl.ds(pl.multiple_of(i * rows, rows), rows), :],
            out_sem.at[lax.rem(i, slots)],
        )

    @pl.loop(0, steps)
    def _(i):
        slot = lax.rem(i, slots)

        @pl.when(i >= slots)
        def _():
            store(i - slots).wait()

        here = pl.ds(pl.multiple_of(i * rows, rows), rows)
        gram = lax.dot_general(
            rt_ref[:, here], cp_ref[...], (((0,), (0,)), ((), ())), preferred_element_type=jnp.float32
        )
        out[slot] = old_ref[here, :] + scaled(gram, tokens)
        store(i).start()

    for k in range(min(slots, steps)):
        store(jnp.int32(steps - 1 - k)).wait()


def step_kernel(n, *refs):
    got, (cp_ref, w_ref, m_ref, new_hbm, new, new_sem) = refs[:n], refs[n:]
    depth, tile = w_ref.shape
    tokens = cp_ref.shape[0]
    extra = got[0][:, tile:].astype(jnp.float32)
    for s in range(1, n):
        extra = extra + got[s][:, tile:].astype(jnp.float32)
    step = 0.25 * (tile * n) / jnp.sum(extra[:, 2 * tokens :], axis=(0, 1), keepdims=True)
    high, low = split(extra[:, :tokens] + extra[:, tokens : 2 * tokens])
    both = jnp.concatenate([high, low.astype(jnp.bfloat16)], axis=0)
    blocks = m_ref.shape[1]
    width = tile // blocks
    for b in range(blocks):
        at = slice(b * width, (b + 1) * width)
        value = jnp.dot(both, cp_ref[:, at], preferred_element_type=jnp.float32)
        grad = scaled(value[:depth] + value[depth:], tokens)
        for s in range(n):
            grad = grad + got[s][:, at].astype(jnp.float32)
        kept = m_ref[:, b : b + 1].astype(jnp.float32)
        new[:, at] = kept * (w_ref[:, at] - step * grad)
    last = pltpu.make_async_copy(new, new_hbm, new_sem)
    last.start()
    last.wait()


def fused(n, hessian_old, tokens, weight, dense_weight, block_mask):
    tile = hessian_old.shape[0]
    held = tokens.shape[0]
    depth = weight.shape[0]
    vmem = pl.BlockSpec(memory_space=pltpu.VMEM)
    dma = pltpu.SemaphoreType.DMA
    hbm = pl.BlockSpec(memory_space=pltpu.HBM)
    parts = 3 if tile % 384 == 0 else 1
    wide = tile + 2 * n * held + 128
    old, colp, rowt, *packs = pl.pallas_call(
        functools.partial(gather_kernel, n, parts),
        out_shape=(
            jax.ShapeDtypeStruct((tile, tile), jnp.float32),
            jax.ShapeDtypeStruct((n, held, tile), jnp.bfloat16),
            jax.ShapeDtypeStruct((n, held, tile), jnp.bfloat16),
        )
        + (jax.ShapeDtypeStruct((depth, wide), jnp.bfloat16),) * n,
        in_specs=[hbm] * 5,
        out_specs=(vmem,) * (3 + n),
        scratch_shapes=[
            pltpu.VMEM((held, tile), jnp.bfloat16),
            pltpu.VMEM((depth, tile), jnp.float32),
            pltpu.VMEM((depth, tile), jnp.float32),
            pltpu.VMEM(block_mask.shape, jnp.int32),
            pltpu.VMEM((depth, tile), jnp.bfloat16),
            pltpu.VMEM((n, depth, tile), jnp.bfloat16),
            pltpu.VMEM((2, 8, 128), jnp.float32),
            pltpu.VMEM((n, depth, wide), jnp.bfloat16),
            dma((4,)),
            dma,
            dma((n,)),
            dma((n,)),
            dma((n,)),
            dma,
            dma((n,)),
            dma((n // 2, 2, n)),
            dma((2, n)),
            dma((n - 1,)),
            dma,
        ],
        compiler_params=pltpu.CompilerParams(
            collective_id=0, has_side_effects=True, vmem_limit_bytes=16 << 20
        ),
    )(*[pltpu.with_memory_space_constraint(x, pltpu.HBM) for x in (hessian_old, tokens, weight, dense_weight, block_mask)])
    colp = colp.reshape(n * held, tile)
    rowt = rowt.reshape(n * held, tile)
    got = [packs[0]] + [
        lax.ppermute(packs[k], "row", [(i, (i + k) % n) for i in range(n)]) for k in range(1, n)
    ]
    rows = 256 if tile % 256 == 0 else 128
    hessian = pl.pallas_call(
        functools.partial(main_kernel, rows),
        out_shape=jax.ShapeDtypeStruct((tile, tile), jnp.float32),
        in_specs=[vmem] * 3,
        out_specs=hbm,
        scratch_shapes=[pltpu.VMEM((3, rows, tile), jnp.float32), dma((3,))],
        compiler_params=pltpu.CompilerParams(vmem_limit_bytes=12 << 20),
        cost_estimate=pl.CostEstimate(
            flops=2 * n * held * tile * tile, bytes_accessed=8 * tile * tile, transcendentals=0
        ),
    )(old, rowt, colp)
    new_weight = pl.pallas_call(
        functools.partial(step_kernel, n),
        out_shape=jax.ShapeDtypeStruct((depth, tile), jnp.float32),
        in_specs=[vmem] * (n + 3),
        out_specs=hbm,
        scratch_shapes=[pltpu.VMEM((depth, tile), jnp.float32), dma],
        compiler_params=pltpu.CompilerParams(vmem_limit_bytes=4 << 20),
    )(*got, colp, weight, block_mask)
    return hessian, new_weight


def solution(mesh):
    n = mesh.shape["row"]

    def on_device(hessian_old, tokens, weight, dense_weight, block_mask):
        tile = hessian_old.shape[0]
        fits = (
            n == mesh.shape["col"]
            and n > 1
            and n % 2 == 0
            and tile == hessian_old.shape[1]
            and tile % 128 == 0
            and tile == block_mask.shape[1] * 128
            and tokens.shape[0] % 16 == 0
            and weight.shape[0] == 16
            and tokens.shape[0] * n % 64 == 0
        )
        args = (hessian_old, tokens, weight, dense_weight, block_mask)
        return fused(n, *args) if fits else general(*args)

    spec = P(("grp", "row"), "col")
    return jax.shard_map(
        on_device, mesh=mesh, in_specs=(spec,) * 5, out_specs=(spec, spec), check_vma=False
    )
```

```python
import functools

import jax
import jax.numpy as jnp
from jax import lax
from jax.experimental import pallas as pl
from jax.experimental.pallas import tpu as pltpu
from jax.sharding import PartitionSpec as P

MESH = pl.DeviceIdType.MESH


def general(hessian_old, tokens, weight, dense_weight, block_mask):
    row_tile = hessian_old.shape[0]
    col_tile = hessian_old.shape[1]
    row_idx = lax.axis_index("row")
    col_idx = lax.axis_index("col")
    col_panel = lax.all_gather(tokens, "row", axis=0, tiled=True)
    features = lax.all_gather(tokens, "col", axis=1, tiled=True)
    row_panel = lax.all_to_all(features, "row", split_axis=1, concat_axis=0, tiled=True)
    gram_tile = lax.dot_general(
        row_panel, col_panel, (((0,), (0,)), ((), ())), preferred_element_type=jnp.float32
    )
    token_count = tokens.shape[0] * lax.axis_size("row")
    hessian = hessian_old + gram_tile / token_count
    row_ids = lax.broadcasted_iota(jnp.int32, (row_tile, col_tile), 0) + row_idx * row_tile
    col_ids = lax.broadcasted_iota(jnp.int32, (row_tile, col_tile), 1) + col_idx * col_tile
    local_trace = jnp.sum(jnp.where(row_ids == col_ids, hessian, jnp.float32(0.0)))
    diag_sum = lax.psum(local_trace, ("row", "col"))
    weight_rows = weight.shape[0]
    block_count = block_mask.shape[1]
    block_width = col_tile // block_count
    kept_mask = (
        block_mask.astype(jnp.float32)[:, :, None] * jnp.ones((1, 1, block_width), jnp.float32)
    ).reshape(weight_rows, col_tile)
    difference = (kept_mask * weight - dense_weight).astype(jnp.bfloat16)
    hess_low = hessian.astype(jnp.bfloat16)
    partial_grad = lax.dot_general(
        lax.all_gather(difference, "row", axis=0, tiled=True),
        hess_low,
        (((1,), (1,)), ((), ())),
        preferred_element_type=jnp.float32,
    )
    spread = lax.all_to_all(partial_grad, "row", split_axis=0, concat_axis=1, tiled=True)
    gradient = lax.psum_scatter(spread, "col", scatter_dimension=1, tiled=True)
    step_size = 0.25 * (row_tile * lax.axis_size("row")) / diag_sum
    new_weight = kept_mask * (weight - step_size * gradient)
    return (hessian, new_weight)


def hail(devices):
    barrier = pltpu.get_barrier_semaphore()
    for device in devices:
        pl.semaphore_signal(barrier, inc=1, device_id=device, device_id_type=MESH)


def meet(count):
    pl.semaphore_wait(pltpu.get_barrier_semaphore(), count)


def remote(src, dst, send_sem, recv_sem, device):
    return pltpu.make_async_remote_copy(
        src_ref=src, dst_ref=dst, send_sem=send_sem, recv_sem=recv_sem,
        device_id=device, device_id_type=MESH,
    )


def scaled(value, count):
    exact = count & (count - 1) == 0
    return value * (1.0 / count) if exact else value / count


def split(value):
    high = value.astype(jnp.bfloat16)
    return high, value - high.astype(jnp.float32)


def swap(index, mask):
    bit = 1
    while bit <= mask:
        if mask & bit:
            index = index + bit - 2 * bit * ((index // bit) % 2)
        bit *= 2
    return index


def gather_kernel(
    n, parts, old_hbm, tok_hbm, w_hbm, d_hbm, m_hbm, old, colp, rowt, *refs
):
    outs, refs = refs[:n], refs[n:]
    (
        tok_ref, w_ref, d_ref, m_ref, diff, rowd, dsum, pack,
        in_sem, old_sem, send_a, recv_a, send_r, send_d, recv_d, send_x, recv_x, send_s, recv_s,
    ) = refs
    g, r, c = lax.axis_index("grp"), lax.axis_index("row"), lax.axis_index("col")
    tile = old.shape[0]
    held = tok_ref.shape[0]
    depth = diff.shape[0]
    loads = [
        pltpu.make_async_copy(src, dst, in_sem.at[i])
        for i, (src, dst) in enumerate([(w_hbm, w_ref), (d_hbm, d_ref), (m_hbm, m_ref), (tok_hbm, tok_ref)])
    ]
    for load in loads:
        load.start()
    others = [lax.rem(r + j, n) for j in range(1, n)]
    beside = [lax.rem(c + j, n) for j in range(1, n)]
    hail([(g, rr, c) for rr in others] + [(g, r, cc) for cc in beside])
    for load in loads:
        load.wait()
    whole = pltpu.make_async_copy(old_hbm, old, old_sem)
    whole.start()
    blocks = m_ref.shape[1]
    width = tile // blocks
    for b in range(blocks):
        at = slice(b * width, (b + 1) * width)
        kept = m_ref[:, b : b + 1].astype(jnp.float32)
        diff[:, at] = (kept * w_ref[:, at] - d_ref[:, at]).astype(jnp.bfloat16)
    meet(len(others) + len(beside))

    root = r == c
    partner = c + 1 - 2 * lax.rem(c, 2)
    partner_dev = (g, r, partner)
    twins = [lax.rem(c + 2 * j, n) for j in range(1, n // 2)]
    even = lax.rem(r, 2) == lax.rem(c, 2)
    twin = jnp.logical_and(even, jnp.logical_not(root))
    mate = partner
    crosses = r // 2 != c // 2
    panels = (rowd, rowt)
    sources = (diff, tok_ref)
    start = lambda copy: copy.start()
    sent = lambda copy: copy.wait_send()

    def direct(rr):
        return jnp.logical_and(rr != r, jnp.logical_not(jnp.logical_and(crosses, rr == mate)))

    def relay(s, act):
        copy = remote(colp.at[s], colp.at[s], send_r.at[s], recv_a.at[s], (g, mate, c))

        @pl.when(s // 2 != r // 2)
        def _():
            act(copy)

    def token_copy(k):
        rr = lax.rem(c + k, n)
        return rr, remote(tok_ref, colp.at[r], send_a.at[k], recv_a.at[r], (g, rr, c))

    diff_copy = remote(diff, rowd.at[r], send_d, recv_d.at[r], (g, c, c))

    def spread(kind, s, src, act):
        for i, cc in enumerate(twins + [partner]):
            act(remote(src, panels[kind].at[s], send_x.at[i, kind, s], recv_x.at[kind, s], (g, r, cc)))

    def spread_on(kind, s, act):
        at = panels[kind].at[s]
        act(remote(at, at, send_x.at[0, kind, s], recv_x.at[kind, s], partner_dev))

    def got_a(s):
        remote(tok_ref, colp.at[s], send_a.at[0], recv_a.at[s], partner_dev).wait_recv()

    def got_x(kind, s):
        spread_on(kind, s, lambda copy: copy.wait_recv())

    def got_diff(s):
        remote(diff, rowd.at[s], send_d, recv_d.at[s], partner_dev).wait_recv()

    late = lax.rem(c, 2) == 1

    def tokens_out(first):
        if first:
            token_copy(0)[1].start()
        for k in range(1, n):
            rr, copy = token_copy(k)

            @pl.when(direct(rr))
            def _():
                copy.start()

    @pl.when(jnp.logical_not(root))
    def _():
        diff_copy.start()

        @pl.when(jnp.logical_not(late))
        def _():
            tokens_out(True)

    @pl.when(root)
    def _():
        spread(0, r, diff, start)
        spread(1, r, tok_ref, start)

    colp[r] = tok_ref[...]

    @pl.when(root)
    def _():
        rowd[r] = diff[...]
        for s in others:
            got_diff(s)
            spread(0, s, rowd.at[s], start)

    @pl.when(root)
    def _():
        tokens_out(False)

    @pl.when(twin)
    def _():
        for i, s in enumerate([r] + others):
            got_x(0, s)
            spread_on(0, s, start)
            if i == 0:
                @pl.when(late)
                def _():
                    tokens_out(True)

    @pl.when(jnp.logical_not(even))
    def _():
        for i, s in enumerate([r] + others):
            got_x(0, s)
            if i == 0:
                @pl.when(late)
                def _():
                    tokens_out(True)

    same = lax.broadcasted_iota(jnp.int32, (width, width), 0) == lax.broadcasted_iota(
        jnp.int32, (width, width), 1
    )

    def diag_to(i, cc):
        return remote(dsum.at[0], dsum.at[1], send_s.at[i], recv_s, (g, r, cc))

    def tokens_step(i):
        s = others[i]

        @pl.when(root)
        def _():
            got_a(s)
            spread(1, s, colp.at[s], start)
            relay(s, start)

        @pl.when(twin)
        def _():
            q = ([r] + others)[i]
            got_x(1, q)
            spread_on(1, q, start)

    whole.wait()
    span = tile // parts
    for p in range(parts):
        at = slice(p * span, (p + 1) * span)
        value = jnp.dot(
            rowd[...].reshape(n * depth, tile), old[:, at].astype(jnp.bfloat16), preferred_element_type=jnp.float32
        )
        pack[:, :, at] = value.astype(jnp.bfloat16).reshape(n, depth, span)
        if p < n - 1:
            tokens_step(p)
    for i in range(parts, n - 1):
        tokens_step(i)

    @pl.when(twin)
    def _():
        got_x(1, others[-1])
        spread_on(1, others[-1], start)

    @pl.when(root)
    def _():
        total = jnp.zeros((8, width), jnp.float32)
        for b in range(blocks):
            at = slice(b * width, (b + 1) * width)
            diag = jnp.where(same, old[at, at], 0.0)
            total = total + jnp.sum(diag.reshape(width // 8, 8, width), axis=0)
        dsum[0] = total
        dsum[1] = total
        for i, cc in enumerate(beside):
            diag_to(i, cc).start()
        for s in range(n):
            rowt[s] = colp[s]

    @pl.when(jnp.logical_not(even))
    def _():
        for s in range(n):
            got_x(1, s)

    mix = lax.dot_general(
        rowd[...].reshape(n * depth, tile), rowt[...].reshape(n * held, tile), (((1,), (1,)), ((), ())),
        preferred_element_type=jnp.float32,
    )
    high, low = split(mix)
    pack[:, :, tile : tile + 2 * n * held] = jnp.concatenate(
        [high.astype(jnp.float32), low], axis=1
    ).astype(jnp.bfloat16).reshape(n, depth, 2 * n * held)
    total = jnp.zeros((n * held, width), jnp.float32)
    for b in range(blocks):
        value = rowt[:, :, b * width : (b + 1) * width].reshape(n * held, width).astype(jnp.float32)
        total = total + value * value
    total = scaled(jnp.sum(total.reshape(n * held // 8, 8, width), axis=0), n * held)

    @pl.when(jnp.logical_not(root))
    def _():
        diag_to(0, partner).wait_recv()

    high, low = split(total + dsum[1])
    both = jnp.concatenate([high.astype(jnp.float32), low], axis=0).astype(jnp.bfloat16)
    for s in range(n):
        pack[s, :, tile + 2 * n * held :] = both
    for k in range(n):
        outs[k][...] = pack[swap(r, k)]

    @pl.when(jnp.logical_not(root))
    def _():
        for s in others:
            got_a(s)
        diff_copy.wait_send()
        token_copy(0)[1].wait_send()

    @pl.when(root)
    def _():
        spread(0, r, diff, sent)
        spread(1, r, tok_ref, sent)
        for s in others:
            spread(0, s, rowd.at[s], sent)
            spread(1, s, colp.at[s], sent)
            relay(s, sent)
        for i, cc in enumerate(beside):
            diag_to(i, cc).wait_send()

    @pl.when(twin)
    def _():
        for kind in (0, 1):
            for s in range(n):
                spread_on(kind, s, sent)

    for k in range(1, n):
        rr, copy = token_copy(k)

        @pl.when(direct(rr))
        def _():
            copy.wait_send()


def main_kernel(rows, old_ref, rt_ref, cp_ref, out_hbm, out, out_sem):
    tile = old_ref.shape[0]
    tokens = rt_ref.shape[0]
    steps = tile // rows
    slots = out.shape[0]

    def store(i):
        return pltpu.make_async_copy(
            out.at[lax.rem(i, slots)],
            out_hbm.at[pl.ds(pl.multiple_of(i * rows, rows), rows), :],
            out_sem.at[lax.rem(i, slots)],
        )

    @pl.loop(0, steps)
    def _(i):
        slot = lax.rem(i, slots)

        @pl.when(i >= slots)
        def _():
            store(i - slots).wait()

        here = pl.ds(pl.multiple_of(i * rows, rows), rows)
        gram = lax.dot_general(
            rt_ref[:, here], cp_ref[...], (((0,), (0,)), ((), ())), preferred_element_type=jnp.float32
        )
        out[slot] = old_ref[here, :] + scaled(gram, tokens)
        store(i).start()

    for k in range(min(slots, steps)):
        store(jnp.int32(steps - 1 - k)).wait()


def step_kernel(n, *refs):
    got, (cp_ref, w_ref, m_ref, new_hbm, new, new_sem) = refs[:n], refs[n:]
    depth, tile = w_ref.shape
    tokens = cp_ref.shape[0]
    extra = got[0][:, tile:].astype(jnp.float32)
    for s in range(1, n):
        extra = extra + got[s][:, tile:].astype(jnp.float32)
    step = 0.25 * (tile * n) / jnp.sum(extra[:, 2 * tokens :], axis=(0, 1), keepdims=True)
    high, low = split(extra[:, :tokens] + extra[:, tokens : 2 * tokens])
    both = jnp.concatenate([high, low.astype(jnp.bfloat16)], axis=0)
    blocks = m_ref.shape[1]
    width = tile // blocks
    for b in range(blocks):
        at = slice(b * width, (b + 1) * width)
        value = jnp.dot(both, cp_ref[:, at], preferred_element_type=jnp.float32)
        grad = scaled(value[:depth] + value[depth:], tokens)
        for s in range(n):
            grad = grad + got[s][:, at].astype(jnp.float32)
        kept = m_ref[:, b : b + 1].astype(jnp.float32)
        new[:, at] = kept * (w_ref[:, at] - step * grad)
    last = pltpu.make_async_copy(new, new_hbm, new_sem)
    last.start()
    last.wait()


def fused(n, hessian_old, tokens, weight, dense_weight, block_mask):
    tile = hessian_old.shape[0]
    held = tokens.shape[0]
    depth = weight.shape[0]
    vmem = pl.BlockSpec(memory_space=pltpu.VMEM)
    dma = pltpu.SemaphoreType.DMA
    hbm = pl.BlockSpec(memory_space=pltpu.HBM)
    parts = 3 if tile % 384 == 0 else 1
    wide = tile + 2 * n * held + 128
    old, colp, rowt, *packs = pl.pallas_call(
        functools.partial(gather_kernel, n, parts),
        out_shape=(
            jax.ShapeDtypeStruct((tile, tile), jnp.float32),
            jax.ShapeDtypeStruct((n, held, tile), jnp.bfloat16),
            jax.ShapeDtypeStruct((n, held, tile), jnp.bfloat16),
        )
        + (jax.ShapeDtypeStruct((depth, wide), jnp.bfloat16),) * n,
        in_specs=[hbm] * 5,
        out_specs=(vmem,) * (3 + n),
        scratch_shapes=[
            pltpu.VMEM((held, tile), jnp.bfloat16),
            pltpu.VMEM((depth, tile), jnp.float32),
            pltpu.VMEM((depth, tile), jnp.float32),
            pltpu.VMEM(block_mask.shape, jnp.int32),
            pltpu.VMEM((depth, tile), jnp.bfloat16),
            pltpu.VMEM((n, depth, tile), jnp.bfloat16),
            pltpu.VMEM((2, 8, 128), jnp.float32),
            pltpu.VMEM((n, depth, wide), jnp.bfloat16),
            dma((4,)),
            dma,
            dma((n,)),
            dma((n,)),
            dma((n,)),
            dma,
            dma((n,)),
            dma((n // 2, 2, n)),
            dma((2, n)),
            dma((n - 1,)),
            dma,
        ],
        compiler_params=pltpu.CompilerParams(
            collective_id=0, has_side_effects=True, vmem_limit_bytes=16 << 20
        ),
    )(*[pltpu.with_memory_space_constraint(x, pltpu.HBM) for x in (hessian_old, tokens, weight, dense_weight, block_mask)])
    colp = colp.reshape(n * held, tile)
    rowt = rowt.reshape(n * held, tile)
    got = [packs[0]] + [
        lax.ppermute(packs[k], "row", [(i, swap(i, k)) for i in range(n)]) for k in range(1, n)
    ]
    rows = 256 if tile % 256 == 0 else 128
    hessian = pl.pallas_call(
        functools.partial(main_kernel, rows),
        out_shape=jax.ShapeDtypeStruct((tile, tile), jnp.float32),
        in_specs=[vmem] * 3,
        out_specs=hbm,
        scratch_shapes=[pltpu.VMEM((3, rows, tile), jnp.float32), dma((3,))],
        compiler_params=pltpu.CompilerParams(vmem_limit_bytes=12 << 20),
        cost_estimate=pl.CostEstimate(
            flops=2 * n * held * tile * tile, bytes_accessed=8 * tile * tile, transcendentals=0
        ),
    )(old, rowt, colp)
    new_weight = pl.pallas_call(
        functools.partial(step_kernel, n),
        out_shape=jax.ShapeDtypeStruct((depth, tile), jnp.float32),
        in_specs=[vmem] * (n + 3),
        out_specs=hbm,
        scratch_shapes=[pltpu.VMEM((depth, tile), jnp.float32), dma],
        compiler_params=pltpu.CompilerParams(vmem_limit_bytes=4 << 20),
    )(*got, colp, weight, block_mask)
    return hessian, new_weight


def solution(mesh):
    n = mesh.shape["row"]

    def on_device(hessian_old, tokens, weight, dense_weight, block_mask):
        tile = hessian_old.shape[0]
        fits = (
            n == mesh.shape["col"]
            and n > 1
            and n & (n - 1) == 0
            and tile == hessian_old.shape[1]
            and tile % 128 == 0
            and tile == block_mask.shape[1] * 128
            and tokens.shape[0] % 16 == 0
            and weight.shape[0] == 16
            and tokens.shape[0] * n % 64 == 0
        )
        args = (hessian_old, tokens, weight, dense_weight, block_mask)
        return fused(n, *args) if fits else general(*args)

    spec = P(("grp", "row"), "col")
    return jax.shard_map(
        on_device, mesh=mesh, in_specs=(spec,) * 5, out_specs=(spec, spec), check_vma=False
    )
```

```python
import functools

import jax
import jax.numpy as jnp
from jax import lax
from jax.experimental import pallas as pl
from jax.experimental.pallas import tpu as pltpu
from jax.sharding import PartitionSpec as P

MESH = pl.DeviceIdType.MESH


def general(hessian_old, tokens, weight, dense_weight, block_mask):
    row_tile = hessian_old.shape[0]
    col_tile = hessian_old.shape[1]
    row_idx = lax.axis_index("row")
    col_idx = lax.axis_index("col")
    col_panel = lax.all_gather(tokens, "row", axis=0, tiled=True)
    features = lax.all_gather(tokens, "col", axis=1, tiled=True)
    row_panel = lax.all_to_all(features, "row", split_axis=1, concat_axis=0, tiled=True)
    gram_tile = lax.dot_general(
        row_panel, col_panel, (((0,), (0,)), ((), ())), preferred_element_type=jnp.float32
    )
    token_count = tokens.shape[0] * lax.axis_size("row")
    hessian = hessian_old + gram_tile / token_count
    row_ids = lax.broadcasted_iota(jnp.int32, (row_tile, col_tile), 0) + row_idx * row_tile
    col_ids = lax.broadcasted_iota(jnp.int32, (row_tile, col_tile), 1) + col_idx * col_tile
    local_trace = jnp.sum(jnp.where(row_ids == col_ids, hessian, jnp.float32(0.0)))
    diag_sum = lax.psum(local_trace, ("row", "col"))
    weight_rows = weight.shape[0]
    block_count = block_mask.shape[1]
    block_width = col_tile // block_count
    kept_mask = (
        block_mask.astype(jnp.float32)[:, :, None] * jnp.ones((1, 1, block_width), jnp.float32)
    ).reshape(weight_rows, col_tile)
    difference = (kept_mask * weight - dense_weight).astype(jnp.bfloat16)
    hess_low = hessian.astype(jnp.bfloat16)
    partial_grad = lax.dot_general(
        lax.all_gather(difference, "row", axis=0, tiled=True),
        hess_low,
        (((1,), (1,)), ((), ())),
        preferred_element_type=jnp.float32,
    )
    spread = lax.all_to_all(partial_grad, "row", split_axis=0, concat_axis=1, tiled=True)
    gradient = lax.psum_scatter(spread, "col", scatter_dimension=1, tiled=True)
    step_size = 0.25 * (row_tile * lax.axis_size("row")) / diag_sum
    new_weight = kept_mask * (weight - step_size * gradient)
    return (hessian, new_weight)


def hail(devices):
    barrier = pltpu.get_barrier_semaphore()
    for device in devices:
        pl.semaphore_signal(barrier, inc=1, device_id=device, device_id_type=MESH)


def meet(count):
    pl.semaphore_wait(pltpu.get_barrier_semaphore(), count)


def remote(src, dst, send_sem, recv_sem, device):
    return pltpu.make_async_remote_copy(
        src_ref=src, dst_ref=dst, send_sem=send_sem, recv_sem=recv_sem,
        device_id=device, device_id_type=MESH,
    )


def scaled(value, count):
    exact = count & (count - 1) == 0
    return value * (1.0 / count) if exact else value / count


def split(value):
    high = value.astype(jnp.bfloat16)
    return high, value - high.astype(jnp.float32)


def swap(index, mask):
    bit = 1
    while bit <= mask:
        if mask & bit:
            index = index + bit - 2 * bit * ((index // bit) % 2)
        bit *= 2
    return index


def gather_kernel(
    n, parts, old_hbm, tok_hbm, w_hbm, d_hbm, m_hbm, old, colp, rowt, *refs
):
    outs, refs = refs[:n], refs[n:]
    (
        tok_ref, w_ref, d_ref, m_ref, diff, rowd, dsum, pack,
        in_sem, old_sem, send_a, recv_a, send_r, send_d, recv_d, send_x, recv_x, send_s, recv_s,
    ) = refs
    g, r, c = lax.axis_index("grp"), lax.axis_index("row"), lax.axis_index("col")
    tile = old.shape[0]
    held = tok_ref.shape[0]
    depth = diff.shape[0]
    loads = [
        pltpu.make_async_copy(src, dst, in_sem.at[i])
        for i, (src, dst) in enumerate([(w_hbm, w_ref), (d_hbm, d_ref), (m_hbm, m_ref), (tok_hbm, tok_ref)])
    ]
    for load in loads:
        load.start()
    others = [lax.rem(r + j, n) for j in range(1, n)]
    beside = [lax.rem(c + j, n) for j in range(1, n)]
    hail([(g, rr, c) for rr in others] + [(g, r, cc) for cc in beside])
    for load in loads:
        load.wait()
    whole = pltpu.make_async_copy(old_hbm, old, old_sem)
    whole.start()
    blocks = m_ref.shape[1]
    width = tile // blocks
    for b in range(blocks):
        at = slice(b * width, (b + 1) * width)
        kept = m_ref[:, b : b + 1].astype(jnp.float32)
        diff[:, at] = (kept * w_ref[:, at] - d_ref[:, at]).astype(jnp.bfloat16)
    meet(len(others) + len(beside))

    root = r == c
    partner = c + 1 - 2 * lax.rem(c, 2)
    partner_dev = (g, r, partner)
    twins = [lax.rem(c + 2 * j, n) for j in range(1, n // 2)]
    even = lax.rem(r, 2) == lax.rem(c, 2)
    twin = jnp.logical_and(even, jnp.logical_not(root))
    mate = partner
    crosses = r // 2 != c // 2
    panels = (rowd, rowt)
    sources = (diff, tok_ref)
    start = lambda copy: copy.start()
    sent = lambda copy: copy.wait_send()

    def direct(rr):
        return jnp.logical_and(rr != r, jnp.logical_not(jnp.logical_and(crosses, rr == mate)))

    def relay(s, act):
        copy = remote(colp.at[s], colp.at[s], send_r.at[s], recv_a.at[s], (g, mate, c))

        @pl.when(s // 2 != r // 2)
        def _():
            act(copy)

    def token_copy(k):
        rr = lax.rem(c + k, n)
        return rr, remote(tok_ref, colp.at[r], send_a.at[k], recv_a.at[r], (g, rr, c))

    diff_copy = remote(diff, rowd.at[r], send_d, recv_d.at[r], (g, c, c))

    def spread(kind, s, src, act):
        for i, cc in enumerate(twins + [partner]):
            act(remote(src, panels[kind].at[s], send_x.at[i, kind, s], recv_x.at[kind, s], (g, r, cc)))

    def spread_on(kind, s, act):
        at = panels[kind].at[s]
        act(remote(at, at, send_x.at[0, kind, s], recv_x.at[kind, s], partner_dev))

    def got_a(s):
        remote(tok_ref, colp.at[s], send_a.at[0], recv_a.at[s], partner_dev).wait_recv()

    def got_x(kind, s):
        spread_on(kind, s, lambda copy: copy.wait_recv())

    def got_diff(s):
        remote(diff, rowd.at[s], send_d, recv_d.at[s], partner_dev).wait_recv()

    late = lax.rem(c, 2) == 1

    def tokens_out(first):
        if first:
            token_copy(0)[1].start()
        for k in range(1, n):
            rr, copy = token_copy(k)

            @pl.when(direct(rr))
            def _():
                copy.start()

    @pl.when(jnp.logical_not(root))
    def _():
        diff_copy.start()

        @pl.when(jnp.logical_not(late))
        def _():
            tokens_out(True)

    @pl.when(root)
    def _():
        spread(0, r, diff, start)
        spread(1, r, tok_ref, start)

    colp[r] = tok_ref[...]

    @pl.when(root)
    def _():
        rowd[r] = diff[...]
        for s in others:
            got_diff(s)
            spread(0, s, rowd.at[s], start)

    @pl.when(root)
    def _():
        tokens_out(False)

    @pl.when(twin)
    def _():
        for i, s in enumerate([r] + others):
            got_x(0, s)
            spread_on(0, s, start)
            if i == 0:
                @pl.when(late)
                def _():
                    tokens_out(True)

    @pl.when(jnp.logical_not(even))
    def _():
        for i, s in enumerate([r] + others):
            got_x(0, s)
            if i == 0:
                @pl.when(late)
                def _():
                    tokens_out(True)

    same = lax.broadcasted_iota(jnp.int32, (width, width), 0) == lax.broadcasted_iota(
        jnp.int32, (width, width), 1
    )

    def diag_to(i, cc):
        return remote(dsum.at[0], dsum.at[1], send_s.at[i], recv_s, (g, r, cc))

    def tokens_step(i):
        s = others[i]

        @pl.when(root)
        def _():
            got_a(s)
            spread(1, s, colp.at[s], start)
            relay(s, start)

        @pl.when(twin)
        def _():
            q = ([r] + others)[i]
            got_x(1, q)
            spread_on(1, q, start)

    whole.wait()
    span = tile // parts
    for p in range(parts):
        at = slice(p * span, (p + 1) * span)
        value = jnp.dot(
            rowd[...].reshape(n * depth, tile), old[:, at].astype(jnp.bfloat16), preferred_element_type=jnp.float32
        )
        pack[:, :, at] = value.astype(jnp.bfloat16).reshape(n, depth, span)
        if p % 2 == 1 and p // 2 < n - 1:
            tokens_step(p // 2)
    for i in range(parts // 2, n - 1):
        tokens_step(i)

    @pl.when(twin)
    def _():
        got_x(1, others[-1])
        spread_on(1, others[-1], start)

    @pl.when(root)
    def _():
        total = jnp.zeros((8, width), jnp.float32)
        for b in range(blocks):
            at = slice(b * width, (b + 1) * width)
            diag = jnp.where(same, old[at, at], 0.0)
            total = total + jnp.sum(diag.reshape(width // 8, 8, width), axis=0)
        dsum[0] = total
        dsum[1] = total
        for i, cc in enumerate(beside):
            diag_to(i, cc).start()
        for s in range(n):
            rowt[s] = colp[s]

    @pl.when(jnp.logical_not(even))
    def _():
        for s in range(n):
            got_x(1, s)

    mix = lax.dot_general(
        rowd[...].reshape(n * depth, tile), rowt[...].reshape(n * held, tile), (((1,), (1,)), ((), ())),
        preferred_element_type=jnp.float32,
    )
    high, low = split(mix)
    pack[:, :, tile : tile + 2 * n * held] = jnp.concatenate(
        [high.astype(jnp.float32), low], axis=1
    ).astype(jnp.bfloat16).reshape(n, depth, 2 * n * held)
    total = jnp.zeros((n * held, width), jnp.float32)
    for b in range(blocks):
        value = rowt[:, :, b * width : (b + 1) * width].reshape(n * held, width).astype(jnp.float32)
        total = total + value * value
    total = scaled(jnp.sum(total.reshape(n * held // 8, 8, width), axis=0), n * held)

    @pl.when(jnp.logical_not(root))
    def _():
        diag_to(0, partner).wait_recv()

    high, low = split(total + dsum[1])
    both = jnp.concatenate([high.astype(jnp.float32), low], axis=0).astype(jnp.bfloat16)
    for s in range(n):
        pack[s, :, tile + 2 * n * held :] = both
    for k in range(n):
        outs[k][...] = pack[swap(r, k)]

    @pl.when(jnp.logical_not(root))
    def _():
        for s in others:
            got_a(s)
        diff_copy.wait_send()
        token_copy(0)[1].wait_send()

    @pl.when(root)
    def _():
        spread(0, r, diff, sent)
        spread(1, r, tok_ref, sent)
        for s in others:
            spread(0, s, rowd.at[s], sent)
            spread(1, s, colp.at[s], sent)
            relay(s, sent)
        for i, cc in enumerate(beside):
            diag_to(i, cc).wait_send()

    @pl.when(twin)
    def _():
        for kind in (0, 1):
            for s in range(n):
                spread_on(kind, s, sent)

    for k in range(1, n):
        rr, copy = token_copy(k)

        @pl.when(direct(rr))
        def _():
            copy.wait_send()


def main_kernel(rows, old_ref, rt_ref, cp_ref, out_hbm, out, out_sem):
    tile = old_ref.shape[0]
    tokens = rt_ref.shape[0]
    steps = tile // rows
    slots = out.shape[0]

    def store(i):
        return pltpu.make_async_copy(
            out.at[lax.rem(i, slots)],
            out_hbm.at[pl.ds(pl.multiple_of(i * rows, rows), rows), :],
            out_sem.at[lax.rem(i, slots)],
        )

    @pl.loop(0, steps)
    def _(i):
        slot = lax.rem(i, slots)

        @pl.when(i >= slots)
        def _():
            store(i - slots).wait()

        here = pl.ds(pl.multiple_of(i * rows, rows), rows)
        gram = lax.dot_general(
            rt_ref[:, here], cp_ref[...], (((0,), (0,)), ((), ())), preferred_element_type=jnp.float32
        )
        out[slot] = old_ref[here, :] + scaled(gram, tokens)
        store(i).start()

    for k in range(min(slots, steps)):
        store(jnp.int32(steps - 1 - k)).wait()


def step_kernel(n, *refs):
    got, (cp_ref, w_ref, m_ref, new_hbm, new, new_sem) = refs[:n], refs[n:]
    depth, tile = w_ref.shape
    tokens = cp_ref.shape[0]
    extra = got[0][:, tile:].astype(jnp.float32)
    for s in range(1, n):
        extra = extra + got[s][:, tile:].astype(jnp.float32)
    step = 0.25 * (tile * n) / jnp.sum(extra[:, 2 * tokens :], axis=(0, 1), keepdims=True)
    high, low = split(extra[:, :tokens] + extra[:, tokens : 2 * tokens])
    both = jnp.concatenate([high, low.astype(jnp.bfloat16)], axis=0)
    blocks = m_ref.shape[1]
    width = tile // blocks
    for b in range(blocks):
        at = slice(b * width, (b + 1) * width)
        value = jnp.dot(both, cp_ref[:, at], preferred_element_type=jnp.float32)
        grad = scaled(value[:depth] + value[depth:], tokens)
        for s in range(n):
            grad = grad + got[s][:, at].astype(jnp.float32)
        kept = m_ref[:, b : b + 1].astype(jnp.float32)
        new[:, at] = kept * (w_ref[:, at] - step * grad)
    last = pltpu.make_async_copy(new, new_hbm, new_sem)
    last.start()
    last.wait()


def fused(n, hessian_old, tokens, weight, dense_weight, block_mask):
    tile = hessian_old.shape[0]
    held = tokens.shape[0]
    depth = weight.shape[0]
    vmem = pl.BlockSpec(memory_space=pltpu.VMEM)
    dma = pltpu.SemaphoreType.DMA
    hbm = pl.BlockSpec(memory_space=pltpu.HBM)
    parts = 6 if tile % 768 == 0 else 1
    wide = tile + 2 * n * held + 128
    old, colp, rowt, *packs = pl.pallas_call(
        functools.partial(gather_kernel, n, parts),
        out_shape=(
            jax.ShapeDtypeStruct((tile, tile), jnp.float32),
            jax.ShapeDtypeStruct((n, held, tile), jnp.bfloat16),
            jax.ShapeDtypeStruct((n, held, tile), jnp.bfloat16),
        )
        + (jax.ShapeDtypeStruct((depth, wide), jnp.bfloat16),) * n,
        in_specs=[hbm] * 5,
        out_specs=(vmem,) * (3 + n),
        scratch_shapes=[
            pltpu.VMEM((held, tile), jnp.bfloat16),
            pltpu.VMEM((depth, tile), jnp.float32),
            pltpu.VMEM((depth, tile), jnp.float32),
            pltpu.VMEM(block_mask.shape, jnp.int32),
            pltpu.VMEM((depth, tile), jnp.bfloat16),
            pltpu.VMEM((n, depth, tile), jnp.bfloat16),
            pltpu.VMEM((2, 8, 128), jnp.float32),
            pltpu.VMEM((n, depth, wide), jnp.bfloat16),
            dma((4,)),
            dma,
            dma((n,)),
            dma((n,)),
            dma((n,)),
            dma,
            dma((n,)),
            dma((n // 2, 2, n)),
            dma((2, n)),
            dma((n - 1,)),
            dma,
        ],
        compiler_params=pltpu.CompilerParams(
            collective_id=0, has_side_effects=True, vmem_limit_bytes=16 << 20
        ),
    )(*[pltpu.with_memory_space_constraint(x, pltpu.HBM) for x in (hessian_old, tokens, weight, dense_weight, block_mask)])
    colp = colp.reshape(n * held, tile)
    rowt = rowt.reshape(n * held, tile)
    got = [packs[0]] + [
        lax.ppermute(packs[k], "row", [(i, swap(i, k)) for i in range(n)]) for k in range(1, n)
    ]
    rows = 128
    hessian = pl.pallas_call(
        functools.partial(main_kernel, rows),
        out_shape=jax.ShapeDtypeStruct((tile, tile), jnp.float32),
        in_specs=[vmem] * 3,
        out_specs=hbm,
        scratch_shapes=[pltpu.VMEM((6, rows, tile), jnp.float32), dma((6,))],
        compiler_params=pltpu.CompilerParams(vmem_limit_bytes=12 << 20),
        cost_estimate=pl.CostEstimate(
            flops=2 * n * held * tile * tile, bytes_accessed=8 * tile * tile, transcendentals=0
        ),
    )(old, rowt, colp)
    new_weight = pl.pallas_call(
        functools.partial(step_kernel, n),
        out_shape=jax.ShapeDtypeStruct((depth, tile), jnp.float32),
        in_specs=[vmem] * (n + 3),
        out_specs=hbm,
        scratch_shapes=[pltpu.VMEM((depth, tile), jnp.float32), dma],
        compiler_params=pltpu.CompilerParams(vmem_limit_bytes=4 << 20),
    )(*got, colp, weight, block_mask)
    return hessian, new_weight


def solution(mesh):
    n = mesh.shape["row"]

    def on_device(hessian_old, tokens, weight, dense_weight, block_mask):
        tile = hessian_old.shape[0]
        fits = (
            n == mesh.shape["col"]
            and n > 1
            and n & (n - 1) == 0
            and tile == hessian_old.shape[1]
            and tile % 128 == 0
            and tile == block_mask.shape[1] * 128
            and tokens.shape[0] % 16 == 0
            and weight.shape[0] == 16
            and tokens.shape[0] * n % 64 == 0
        )
        args = (hessian_old, tokens, weight, dense_weight, block_mask)
        return fused(n, *args) if fits else general(*args)

    spec = P(("grp", "row"), "col")
    return jax.shard_map(
        on_device, mesh=mesh, in_specs=(spec,) * 5, out_specs=(spec, spec), check_vma=False
    )
```

```python
import functools

import jax
import jax.numpy as jnp
from jax import lax
from jax.experimental import pallas as pl
from jax.experimental.pallas import tpu as pltpu
from jax.sharding import PartitionSpec as P

MESH = pl.DeviceIdType.MESH


def general(hessian_old, tokens, weight, dense_weight, block_mask):
    row_tile = hessian_old.shape[0]
    col_tile = hessian_old.shape[1]
    row_idx = lax.axis_index("row")
    col_idx = lax.axis_index("col")
    col_panel = lax.all_gather(tokens, "row", axis=0, tiled=True)
    features = lax.all_gather(tokens, "col", axis=1, tiled=True)
    row_panel = lax.all_to_all(features, "row", split_axis=1, concat_axis=0, tiled=True)
    gram_tile = lax.dot_general(
        row_panel, col_panel, (((0,), (0,)), ((), ())), preferred_element_type=jnp.float32
    )
    token_count = tokens.shape[0] * lax.axis_size("row")
    hessian = hessian_old + gram_tile / token_count
    row_ids = lax.broadcasted_iota(jnp.int32, (row_tile, col_tile), 0) + row_idx * row_tile
    col_ids = lax.broadcasted_iota(jnp.int32, (row_tile, col_tile), 1) + col_idx * col_tile
    local_trace = jnp.sum(jnp.where(row_ids == col_ids, hessian, jnp.float32(0.0)))
    diag_sum = lax.psum(local_trace, ("row", "col"))
    weight_rows = weight.shape[0]
    block_count = block_mask.shape[1]
    block_width = col_tile // block_count
    kept_mask = (
        block_mask.astype(jnp.float32)[:, :, None] * jnp.ones((1, 1, block_width), jnp.float32)
    ).reshape(weight_rows, col_tile)
    difference = (kept_mask * weight - dense_weight).astype(jnp.bfloat16)
    hess_low = hessian.astype(jnp.bfloat16)
    partial_grad = lax.dot_general(
        lax.all_gather(difference, "row", axis=0, tiled=True),
        hess_low,
        (((1,), (1,)), ((), ())),
        preferred_element_type=jnp.float32,
    )
    spread = lax.all_to_all(partial_grad, "row", split_axis=0, concat_axis=1, tiled=True)
    gradient = lax.psum_scatter(spread, "col", scatter_dimension=1, tiled=True)
    step_size = 0.25 * (row_tile * lax.axis_size("row")) / diag_sum
    new_weight = kept_mask * (weight - step_size * gradient)
    return (hessian, new_weight)


def hail(devices):
    barrier = pltpu.get_barrier_semaphore()
    for device in devices:
        pl.semaphore_signal(barrier, inc=1, device_id=device, device_id_type=MESH)


def meet(count):
    pl.semaphore_wait(pltpu.get_barrier_semaphore(), count)


def remote(src, dst, send_sem, recv_sem, device):
    return pltpu.make_async_remote_copy(
        src_ref=src, dst_ref=dst, send_sem=send_sem, recv_sem=recv_sem,
        device_id=device, device_id_type=MESH,
    )


def scaled(value, count):
    exact = count & (count - 1) == 0
    return value * (1.0 / count) if exact else value / count


def split(value):
    high = value.astype(jnp.bfloat16)
    return high, value - high.astype(jnp.float32)


def swap(index, mask):
    bit = 1
    while bit <= mask:
        if mask & bit:
            index = index + bit - 2 * bit * ((index // bit) % 2)
        bit *= 2
    return index


def gather_kernel(
    n, parts, old_hbm, tok_hbm, w_hbm, d_hbm, m_hbm, old, colp, rowt, *refs
):
    outs, refs = refs[:n], refs[n:]
    (
        tok_ref, w_ref, d_ref, m_ref, diff, rowd, dsum, pack,
        in_sem, old_sem, send_a, recv_a, send_r, send_d, recv_d, send_x, recv_x, send_s, recv_s,
    ) = refs
    g, r, c = lax.axis_index("grp"), lax.axis_index("row"), lax.axis_index("col")
    tile = old.shape[0]
    held = tok_ref.shape[0]
    depth = diff.shape[0]
    loads = [
        pltpu.make_async_copy(src, dst, in_sem.at[i])
        for i, (src, dst) in enumerate([(w_hbm, w_ref), (d_hbm, d_ref), (m_hbm, m_ref), (tok_hbm, tok_ref)])
    ]
    for load in loads:
        load.start()
    others = [lax.rem(r + j, n) for j in range(1, n)]
    beside = [lax.rem(c + j, n) for j in range(1, n)]
    hail([(g, rr, c) for rr in others] + [(g, r, cc) for cc in beside])
    for load in loads:
        load.wait()
    whole = pltpu.make_async_copy(old_hbm, old, old_sem)
    whole.start()
    blocks = m_ref.shape[1]
    width = tile // blocks
    for b in range(blocks):
        at = slice(b * width, (b + 1) * width)
        kept = m_ref[:, b : b + 1].astype(jnp.float32)
        diff[:, at] = (kept * w_ref[:, at] - d_ref[:, at]).astype(jnp.bfloat16)
    meet(len(others) + len(beside))

    root = r == c
    partner = c + 1 - 2 * lax.rem(c, 2)
    partner_dev = (g, r, partner)
    twins = [lax.rem(c + 2 * j, n) for j in range(1, n // 2)]
    even = lax.rem(r, 2) == lax.rem(c, 2)
    twin = jnp.logical_and(even, jnp.logical_not(root))
    mate = partner
    crosses = r // 2 != c // 2
    panels = (rowd, rowt)
    sources = (diff, tok_ref)
    start = lambda copy: copy.start()
    sent = lambda copy: copy.wait_send()

    def direct(rr):
        return jnp.logical_and(rr != r, jnp.logical_not(jnp.logical_and(crosses, rr == mate)))

    def relay(s, act):
        copy = remote(colp.at[s], colp.at[s], send_r.at[s], recv_a.at[s], (g, mate, c))

        @pl.when(s // 2 != r // 2)
        def _():
            act(copy)

    def token_copy(k):
        rr = lax.rem(c + k, n)
        return rr, remote(tok_ref, colp.at[r], send_a.at[k], recv_a.at[r], (g, rr, c))

    diff_copy = remote(diff, rowd.at[r], send_d, recv_d.at[r], (g, c, c))

    def spread(kind, s, src, act):
        for i, cc in enumerate(twins + [partner]):
            act(remote(src, panels[kind].at[s], send_x.at[i, kind, s], recv_x.at[kind, s], (g, r, cc)))

    def spread_on(kind, s, act):
        at = panels[kind].at[s]
        act(remote(at, at, send_x.at[0, kind, s], recv_x.at[kind, s], partner_dev))

    def got_a(s):
        remote(tok_ref, colp.at[s], send_a.at[0], recv_a.at[s], partner_dev).wait_recv()

    def got_x(kind, s):
        spread_on(kind, s, lambda copy: copy.wait_recv())

    def got_diff(s):
        remote(diff, rowd.at[s], send_d, recv_d.at[s], partner_dev).wait_recv()

    late = jnp.logical_and(lax.rem(c, 2) == 1, crosses)

    def tokens_out(first):
        if first:
            token_copy(0)[1].start()
        for k in range(1, n):
            rr, copy = token_copy(k)

            @pl.when(direct(rr))
            def _():
                copy.start()

    @pl.when(jnp.logical_not(root))
    def _():
        diff_copy.start()

        @pl.when(jnp.logical_not(late))
        def _():
            tokens_out(True)

    @pl.when(root)
    def _():
        spread(0, r, diff, start)
        spread(1, r, tok_ref, start)

    colp[r] = tok_ref[...]

    @pl.when(root)
    def _():
        rowd[r] = diff[...]
        for s in others:
            got_diff(s)
            spread(0, s, rowd.at[s], start)

    @pl.when(root)
    def _():
        tokens_out(False)

    @pl.when(twin)
    def _():
        for i, s in enumerate([r] + others):
            got_x(0, s)
            spread_on(0, s, start)
            if i == 0:
                @pl.when(late)
                def _():
                    tokens_out(True)

    @pl.when(jnp.logical_not(even))
    def _():
        for i, s in enumerate([r] + others):
            got_x(0, s)
            if i == 0:
                @pl.when(late)
                def _():
                    tokens_out(True)

    same = lax.broadcasted_iota(jnp.int32, (width, width), 0) == lax.broadcasted_iota(
        jnp.int32, (width, width), 1
    )

    def diag_to(i, cc):
        return remote(dsum.at[0], dsum.at[1], send_s.at[i], recv_s, (g, r, cc))

    def tokens_step(i):
        s = others[i]

        @pl.when(root)
        def _():
            got_a(s)
            spread(1, s, colp.at[s], start)
            relay(s, start)

        @pl.when(twin)
        def _():
            q = ([r] + others)[i]
            got_x(1, q)
            spread_on(1, q, start)

    whole.wait()
    span = tile // parts
    for p in range(parts):
        at = slice(p * span, (p + 1) * span)
        value = jnp.dot(
            rowd[...].reshape(n * depth, tile), old[:, at].astype(jnp.bfloat16), preferred_element_type=jnp.float32
        )
        pack[:, :, at] = value.astype(jnp.bfloat16).reshape(n, depth, span)
        if p % 2 == 1 and p // 2 < n - 1:
            tokens_step(p // 2)
    for i in range(parts // 2, n - 1):
        tokens_step(i)

    @pl.when(twin)
    def _():
        got_x(1, others[-1])
        spread_on(1, others[-1], start)

    @pl.when(root)
    def _():
        total = jnp.zeros((8, width), jnp.float32)
        for b in range(blocks):
            at = slice(b * width, (b + 1) * width)
            diag = jnp.where(same, old[at, at], 0.0)
            total = total + jnp.sum(diag.reshape(width // 8, 8, width), axis=0)
        dsum[0] = total
        dsum[1] = total
        for i, cc in enumerate(beside):
            diag_to(i, cc).start()
        for s in range(n):
            rowt[s] = colp[s]

    @pl.when(jnp.logical_not(even))
    def _():
        for s in range(n):
            got_x(1, s)

    mix = lax.dot_general(
        rowd[...].reshape(n * depth, tile), rowt[...].reshape(n * held, tile), (((1,), (1,)), ((), ())),
        preferred_element_type=jnp.float32,
    )
    high, low = split(mix)
    pack[:, :, tile : tile + 2 * n * held] = jnp.concatenate(
        [high.astype(jnp.float32), low], axis=1
    ).astype(jnp.bfloat16).reshape(n, depth, 2 * n * held)
    total = jnp.zeros((n * held, width), jnp.float32)
    for b in range(blocks):
        value = rowt[:, :, b * width : (b + 1) * width].reshape(n * held, width).astype(jnp.float32)
        total = total + value * value
    total = scaled(jnp.sum(total.reshape(n * held // 8, 8, width), axis=0), n * held)

    @pl.when(jnp.logical_not(root))
    def _():
        diag_to(0, partner).wait_recv()

    high, low = split(total + dsum[1])
    both = jnp.concatenate([high.astype(jnp.float32), low], axis=0).astype(jnp.bfloat16)
    for s in range(n):
        pack[s, :, tile + 2 * n * held :] = both
    for k in range(n):
        outs[k][...] = pack[swap(r, k)]

    @pl.when(jnp.logical_not(root))
    def _():
        for s in others:
            got_a(s)
        diff_copy.wait_send()
        token_copy(0)[1].wait_send()

    @pl.when(root)
    def _():
        spread(0, r, diff, sent)
        spread(1, r, tok_ref, sent)
        for s in others:
            spread(0, s, rowd.at[s], sent)
            spread(1, s, colp.at[s], sent)
            relay(s, sent)
        for i, cc in enumerate(beside):
            diag_to(i, cc).wait_send()

    @pl.when(twin)
    def _():
        for kind in (0, 1):
            for s in range(n):
                spread_on(kind, s, sent)

    for k in range(1, n):
        rr, copy = token_copy(k)

        @pl.when(direct(rr))
        def _():
            copy.wait_send()


def main_kernel(rows, old_ref, rt_ref, cp_ref, out_hbm, out, out_sem):
    tile = old_ref.shape[0]
    tokens = rt_ref.shape[0]
    steps = tile // rows
    slots = out.shape[0]

    def store(i):
        return pltpu.make_async_copy(
            out.at[lax.rem(i, slots)],
            out_hbm.at[pl.ds(pl.multiple_of(i * rows, rows), rows), :],
            out_sem.at[lax.rem(i, slots)],
        )

    @pl.loop(0, steps)
    def _(i):
        slot = lax.rem(i, slots)

        @pl.when(i >= slots)
        def _():
            store(i - slots).wait()

        here = pl.ds(pl.multiple_of(i * rows, rows), rows)
        gram = lax.dot_general(
            rt_ref[:, here], cp_ref[...], (((0,), (0,)), ((), ())), preferred_element_type=jnp.float32
        )
        out[slot] = old_ref[here, :] + scaled(gram, tokens)
        store(i).start()

    for k in range(min(slots, steps)):
        store(jnp.int32(steps - 1 - k)).wait()


def step_kernel(n, *refs):
    got, (cp_ref, w_ref, m_ref, new_hbm, new, new_sem) = refs[:n], refs[n:]
    depth, tile = w_ref.shape
    tokens = cp_ref.shape[0]
    extra = got[0][:, tile:].astype(jnp.float32)
    for s in range(1, n):
        extra = extra + got[s][:, tile:].astype(jnp.float32)
    step = 0.25 * (tile * n) / jnp.sum(extra[:, 2 * tokens :], axis=(0, 1), keepdims=True)
    high, low = split(extra[:, :tokens] + extra[:, tokens : 2 * tokens])
    both = jnp.concatenate([high, low.astype(jnp.bfloat16)], axis=0)
    blocks = m_ref.shape[1]
    width = tile // blocks
    stops = [0, blocks] if blocks == 1 else [0, (blocks + 1) // 2, blocks]
    copies = []
    for b in range(blocks):
        at = slice(b * width, (b + 1) * width)
        value = jnp.dot(both, cp_ref[:, at], preferred_element_type=jnp.float32)
        grad = scaled(value[:depth] + value[depth:], tokens)
        for s in range(n):
            grad = grad + got[s][:, at].astype(jnp.float32)
        kept = m_ref[:, b : b + 1].astype(jnp.float32)
        new[:, at] = kept * (w_ref[:, at] - step * grad)
        if b + 1 in stops:
            done = slice(stops[stops.index(b + 1) - 1] * width, (b + 1) * width)
            copy = pltpu.make_async_copy(new.at[:, done], new_hbm.at[:, done], new_sem.at[len(copies)])
            copy.start()
            copies.append(copy)
    for copy in copies:
        copy.wait()


def fused(n, hessian_old, tokens, weight, dense_weight, block_mask):
    tile = hessian_old.shape[0]
    held = tokens.shape[0]
    depth = weight.shape[0]
    vmem = pl.BlockSpec(memory_space=pltpu.VMEM)
    dma = pltpu.SemaphoreType.DMA
    hbm = pl.BlockSpec(memory_space=pltpu.HBM)
    parts = 6 if tile % 768 == 0 else 1
    wide = tile + 2 * n * held + 128
    old, colp, rowt, *packs = pl.pallas_call(
        functools.partial(gather_kernel, n, parts),
        out_shape=(
            jax.ShapeDtypeStruct((tile, tile), jnp.float32),
            jax.ShapeDtypeStruct((n, held, tile), jnp.bfloat16),
            jax.ShapeDtypeStruct((n, held, tile), jnp.bfloat16),
        )
        + (jax.ShapeDtypeStruct((depth, wide), jnp.bfloat16),) * n,
        in_specs=[hbm] * 5,
        out_specs=(vmem,) * (3 + n),
        scratch_shapes=[
            pltpu.VMEM((held, tile), jnp.bfloat16),
            pltpu.VMEM((depth, tile), jnp.float32),
            pltpu.VMEM((depth, tile), jnp.float32),
            pltpu.VMEM(block_mask.shape, jnp.int32),
            pltpu.VMEM((depth, tile), jnp.bfloat16),
            pltpu.VMEM((n, depth, tile), jnp.bfloat16),
            pltpu.VMEM((2, 8, 128), jnp.float32),
            pltpu.VMEM((n, depth, wide), jnp.bfloat16),
            dma((4,)),
            dma,
            dma((n,)),
            dma((n,)),
            dma((n,)),
            dma,
            dma((n,)),
            dma((n // 2, 2, n)),
            dma((2, n)),
            dma((n - 1,)),
            dma,
        ],
        compiler_params=pltpu.CompilerParams(
            collective_id=0, has_side_effects=True, vmem_limit_bytes=16 << 20
        ),
    )(*[pltpu.with_memory_space_constraint(x, pltpu.HBM) for x in (hessian_old, tokens, weight, dense_weight, block_mask)])
    colp = colp.reshape(n * held, tile)
    rowt = rowt.reshape(n * held, tile)
    got = [packs[0]] + [
        lax.ppermute(packs[k], "row", [(i, swap(i, k)) for i in range(n)]) for k in range(1, n)
    ]
    rows = 128
    hessian = pl.pallas_call(
        functools.partial(main_kernel, rows),
        out_shape=jax.ShapeDtypeStruct((tile, tile), jnp.float32),
        in_specs=[vmem] * 3,
        out_specs=hbm,
        scratch_shapes=[pltpu.VMEM((6, rows, tile), jnp.float32), dma((6,))],
        compiler_params=pltpu.CompilerParams(vmem_limit_bytes=12 << 20),
        cost_estimate=pl.CostEstimate(
            flops=2 * n * held * tile * tile, bytes_accessed=8 * tile * tile, transcendentals=0
        ),
    )(old, rowt, colp)
    new_weight = pl.pallas_call(
        functools.partial(step_kernel, n),
        out_shape=jax.ShapeDtypeStruct((depth, tile), jnp.float32),
        in_specs=[vmem] * (n + 3),
        out_specs=hbm,
        scratch_shapes=[pltpu.VMEM((depth, tile), jnp.float32), dma((2,))],
        compiler_params=pltpu.CompilerParams(vmem_limit_bytes=4 << 20),
    )(*got, colp, weight, block_mask)
    return hessian, new_weight


def solution(mesh):
    n = mesh.shape["row"]

    def on_device(hessian_old, tokens, weight, dense_weight, block_mask):
        tile = hessian_old.shape[0]
        fits = (
            n == mesh.shape["col"]
            and n > 1
            and n & (n - 1) == 0
            and tile == hessian_old.shape[1]
            and tile % 128 == 0
            and tile == block_mask.shape[1] * 128
            and tokens.shape[0] % 16 == 0
            and weight.shape[0] == 16
            and tokens.shape[0] * n % 64 == 0
        )
        args = (hessian_old, tokens, weight, dense_weight, block_mask)
        return fused(n, *args) if fits else general(*args)

    spec = P(("grp", "row"), "col")
    return jax.shard_map(
        on_device, mesh=mesh, in_specs=(spec,) * 5, out_specs=(spec, spec), check_vma=False
    )
```
